256 devices in a mesh: parts: 4 (over y, x), rows: 64 (over z, core).
Axes of the slice: x: 2, y: 2, z: 32, core: 2. Of those that a mesh axis runs over, the one named last changes fastest.
The devices are a block of a 4x8x32 slice.
Arguments:
- features: bfloat16 [1024, 256, 512], P(('parts', 'rows')), parts along dimension 0, may hold values from -10 to 10, as said below
- grad_out: bfloat16 [1024, 256, 512], P(('parts', 'rows')), parts along dimension 0, may hold values from -11 to 11, as said below
- filters: bfloat16 [512, 3, 3, 512], replicated, may hold values from -0.09375 to 0.09375
- norm_gain: float32 [512], replicated, may hold values from 0.25 to 1.75
- norm_bias: float32 [512], replicated, may hold values from -1 to 1
Outputs:
- grad_in: bfloat16 [1024, 256, 512], P(('parts', 'rows')), parts along dimension 0
- filter_grad: float32 [2048, 3, 3, 512], P(('parts', 'rows')), parts along dimension 0
- gain_grad: float32 [2048], P('parts'), parts along dimension 0
- bias_grad: float32 [2048], P('parts'), parts along dimension 0
The draws below stay inside these ranges and needn't reach their ends.
There are 4 independent parts, one for each index of `parts`. The reference program is written for one: setup_inputs(seed, part) draws one part's arguments, and reference() takes and returns one part's arrays. A program takes and returns all parts, laid end to end along the dimension named above; an argument that names none is the same for every part. Nothing has to cross between parts.
Inputs may be any that keep to these rules, and one draw needn't show every extreme that they name: `features`: each image row has its own offset and spread for each group. `grad_out`: each image row and channel has its own offset.
All inputs are finite; a program needn't handle non-finite values.
Results may differ from the reference program's by a relative error of at most 0.0005.
Values may be sent and summed in bfloat16 or wider, within the bound.
No kernel may reach another device: no remote copies, remote signals or barrier semaphores. Data moves between devices by JAX's collectives and lax.ppermute only.
A program may use at most 128 MiB of HBM per device.

```python
import math
import jax
import jax.numpy as jnp
from jax import lax

C = 512
GROUPS = 32
COLS = 256
HEIGHT = 256


def draw_features(key, part):
    key_noise = jax.random.fold_in(key, 11)
    key_offset = jax.random.fold_in(key, 12)
    key_spread = jax.random.fold_in(key, 13)
    normal_draw = jnp.clip(jax.random.normal(key_noise, (HEIGHT, COLS, C), jnp.float32), -4.0, 4.0)
    offset = jax.random.uniform(key_offset, (HEIGHT, 1, GROUPS), jnp.float32, -1.0, 1.0)
    spread = jnp.exp(jax.random.uniform(key_spread, (HEIGHT, 1, GROUPS), jnp.float32, math.log(0.5), math.log(2.0)))
    offset = jnp.repeat(offset, C // GROUPS, axis=2)
    spread = jnp.repeat(spread, C // GROUPS, axis=2)
    return (offset + spread * normal_draw).astype(jnp.bfloat16)


def draw_grad_out(key, part):
    key_noise = jax.random.fold_in(key, 21)
    key_offset = jax.random.fold_in(key, 22)
    normal_draw = jnp.clip(jax.random.normal(key_noise, (HEIGHT, COLS, C), jnp.float32), -4.0, 4.0)
    offset = jax.random.uniform(key_offset, (HEIGHT, 1, C), jnp.float32, -1.0, 3.0)
    return (offset + normal_draw).astype(jnp.bfloat16)


def centred(own_key, shape, scale, limit, held_as=jnp.bfloat16):
    entries = scale * jax.random.normal(own_key, shape, jnp.float32)
    return jnp.clip(entries, min=-limit, max=limit).astype(held_as)


def setup_inputs(seed: int = 0, part: int = 0) -> dict:
    streams_of = jax.random.split(jax.random.key(seed), 6)
    part_splits = jax.random.split(jax.random.fold_in(streams_of[5], part), 6)
    features = draw_features(jax.random.fold_in(jax.random.fold_in(streams_of[5], part), 71), part)
    grad_out = draw_grad_out(jax.random.fold_in(jax.random.fold_in(streams_of[5], part), 71), part)
    filters = centred(streams_of[2], (C, 3, 3, C), (9 * C) ** -0.5, 0.09375)
    norm_gain = jnp.clip(1.0 + 0.15 * jax.random.normal(streams_of[3], (C,), jnp.float32), 0.25, 1.75)
    norm_bias = jnp.clip(jax.random.uniform(streams_of[4], (C,), jnp.float32, -1.0, 1.0), -1.0, 1.0)
    return dict(features=features, grad_out=grad_out, filters=filters, norm_gain=norm_gain, norm_bias=norm_bias)


epsilon = 1e-06

def expand(values, channels):
    groups = values.shape[0]
    return jnp.broadcast_to(values[:, None], (groups, channels // groups)).reshape(channels)

def group_total(values):
    return values.reshape(GROUPS, -1).sum(axis=1)

def reference(features, grad_out, filters, norm_gain, norm_bias):
    height, columns, channels = features.shape
    pixels = height * columns
    members = pixels * (channels // GROUPS)
    widened = features.astype(jnp.float32)
    group_mean = group_total(lax.optimization_barrier(jnp.sum(widened, axis=(0, 1)))) / members
    centered = widened - expand(group_mean, channels)
    group_var = group_total(lax.optimization_barrier(jnp.sum(centered * centered, axis=(0, 1)))) / members
    inv_std = lax.rsqrt(group_var + epsilon)
    normalized = centered * expand(inv_std, channels)
    normed = normalized * norm_gain + norm_bias
    sigmoid_z = jax.nn.sigmoid(normed)
    activation = (normed * sigmoid_z).astype(jnp.bfloat16)
    flat_act = activation.reshape(-1, channels)
    padded = jnp.pad(grad_out, ((1, 1), (1, 1), (0, 0)))
    grad_act = jnp.zeros((pixels, channels), jnp.float32)
    pieces = []
    for tap_row in range(3):
        for tap_col in range(3):
            window = padded[2 - tap_row:2 - tap_row + height, 2 - tap_col:2 - tap_col + columns].reshape(-1, channels)
            grad_act = grad_act + jnp.dot(window, filters[:, tap_row, tap_col, :], preferred_element_type=jnp.float32)
            pieces.append(lax.dot_general(window, flat_act, (((0,), (0,)), ((), ())), preferred_element_type=jnp.float32))
    filter_grad = jnp.stack(pieces, axis=1).reshape(channels, 3, 3, channels) / pixels
    grad_pre = grad_act.reshape(height, columns, channels) * (sigmoid_z * (1.0 + normed * (1.0 - sigmoid_z)))
    bias_grad = lax.optimization_barrier(jnp.sum(grad_pre, axis=(0, 1)))
    gain_grad = lax.optimization_barrier(jnp.sum(grad_pre * normalized, axis=(0, 1)))
    mean_grad = group_total(norm_gain * bias_grad) / members
    mean_cross = group_total(norm_gain * gain_grad) / members
    grad_in = expand(inv_std, channels) * (grad_pre * norm_gain - expand(mean_grad, channels) - normalized * expand(mean_cross, channels))
    return (grad_in.astype(jnp.bfloat16), filter_grad, gain_grad, bias_grad)
```

```python
import functools

import jax
import jax.numpy as jnp
from jax import lax
from jax.experimental import pallas as pl
from jax.experimental.pallas import tpu as pltpu
from jax.sharding import Mesh
from jax.sharding import PartitionSpec as P


GROUPS = 32
CHIPS = "chip"
CORES = "core"
ROWS = ("chip", "core")
PARTS_ROWS = ("parts", "chip", "core")
CORES_PER_CHIP = 2
SEND_SCALE = 1.0 / 128.0

epsilon = 1e-06
f32, bf16, f16 = jnp.float32, jnp.bfloat16, jnp.float16

FAR = (-15, 15)
MIDDLE = (-12, -9, -6, -3, 0, 3, 6, 9, 12)
HUBS = FAR + MIDDLE
SETS = {
    "far": (FAR[0] + 1, FAR[1] + 1, FAR[1] - 1),
    "left": tuple(h + 1 for h in MIDDLE),
    "right": tuple(h - 1 for h in MIDDLE),
    "kept": HUBS + (0,),
}
BLOCK = 3


def swap_cores(x):
    return lax.ppermute(x, CORES, [(0, 1), (1, 0)])


def along(x, step):
    chips = lax.axis_size(CHIPS)
    return lax.ppermute(x, CHIPS, [(i, (i + step) % chips) for i in range(chips)])


def from_all(vector, axes):
    copies = jnp.broadcast_to(vector, (lax.axis_size(axes), *vector.shape))
    return lax.all_to_all(copies, axes, split_axis=0, concat_axis=0, tiled=True)


def with_halo(block):
    count = lax.axis_size(ROWS)
    forward = [(i, i + 1) for i in range(count - 1)]
    backward = [(target, source) for source, target in forward]
    low = lax.ppermute(block[-1:], ROWS, forward)
    high = lax.ppermute(block[:1], ROWS, backward)
    return jnp.concatenate([low, block, high], axis=0)


def expand(values, channels):
    groups = values.shape[0]
    return jnp.broadcast_to(values[:, None], (groups, channels // groups)).reshape(channels)


def group_total(values):
    return values.reshape(GROUPS, -1).sum(axis=1)


def picked_channels(places, channels, core):
    chips = lax.axis_size(CHIPS)
    own = channels // (chips * CORES_PER_CHIP)
    column = jnp.arange(len(places) * own)
    place = jnp.repeat(jnp.array(places), own)
    owner = (lax.axis_index(CHIPS) - place + 2 * chips) % chips
    channel = (owner * CORES_PER_CHIP + core) * own + column % own
    return (jnp.arange(channels)[:, None] == channel[None, :]).astype(bf16)


def window_kernel(pixels, columns, own, *refs):
    *sides, out_ref = refs
    for side, ref in enumerate(sides):
        x = ref[...].astype(f32)
        rows, flat = x.shape
        at = lax.broadcasted_iota(jnp.int32, x.shape, 1) % columns
        shifted = (
            jnp.where(at == columns - 1, 0.0, pltpu.roll(x, flat - 1, 1)),
            x,
            jnp.where(at == 0, 0.0, pltpu.roll(x, 1, 1)),
        )
        for tap_row in range(3):
            lo = (2 - tap_row) * columns
            for tap_col in range(3):
                part = shifted[tap_col][:, lo : lo + pixels].reshape(rows // own, own, pixels)
                out_ref[:, tap_row * 3 + tap_col, :, side * pixels : (side + 1) * pixels] = part.astype(bf16)


def windows_of(sides, start, count, pixels, columns, own):
    flat = sides[0].shape[1]
    first = start // BLOCK
    return pl.pallas_call(
        functools.partial(window_kernel, pixels, columns, own),
        grid=(count // BLOCK,),
        in_specs=[pl.BlockSpec((BLOCK * own, flat), lambda i: (i + first, 0)) for _ in sides],
        out_specs=pl.BlockSpec((BLOCK, 9, own, len(sides) * pixels), lambda i: (i, 0, 0, 0)),
        out_shape=jax.ShapeDtypeStruct((count, 9, own, len(sides) * pixels), bf16),
        cost_estimate=pl.CostEstimate(
            flops=count * 10**7, bytes_accessed=20 * count * own * flat, transcendentals=0
        ),
    )(*sides)


def steps(features, grad_out, filters, norm_gain, norm_bias):
    height, columns, channels = features.shape
    chips = lax.axis_size(CHIPS)
    pixels = height * columns
    all_pixels = pixels * chips * CORES_PER_CHIP
    members = all_pixels * (channels // GROUPS)
    own = channels // (chips * CORES_PER_CHIP)
    core = lax.axis_index(CORES)

    widened = features.astype(f32)
    partial_value = jnp.sum(widened, axis=(0, 1))
    squares = jnp.sum(widened * widened, axis=(0, 1))
    stats = jnp.concatenate([group_total(partial_value), group_total(squares)])
    all_stats = from_all(stats, ROWS)

    extended = with_halo(grad_out)
    partner_features = swap_cores(features)
    flat = extended.reshape(-1, channels)
    places = sum(SETS.values(), ())
    chosen = jnp.concatenate(
        [picked_channels(places, channels, core), picked_channels(places, channels, 1 - core)], axis=1
    )
    rows = lax.dot_general(chosen, flat, (((0,), (1,)), ((), ())), preferred_element_type=f32).astype(bf16)
    half = len(places) * own
    both = (rows[:half], swap_cores(rows[half:]))
    windows, at = {}, 0
    for name, set_places in SETS.items():
        windows[name] = windows_of(both, at, len(set_places), pixels, columns, own)
        at += len(set_places)
    all_stats, windows, partner_features = lax.optimization_barrier((all_stats, windows, partner_features))

    stats = all_stats.sum(axis=0)
    group_mean = stats[:GROUPS] / members
    group_var = stats[GROUPS:] / members - group_mean * group_mean
    inv_std = lax.rsqrt(group_var + epsilon)
    mean_of, std_of = expand(group_mean, channels), expand(inv_std, channels)

    def activated(block):
        normalized = (block.astype(f32) - mean_of) * std_of
        normed = normalized * norm_gain + norm_bias
        return normalized, normed, jax.nn.sigmoid(normed)

    normalized, normed, sigmoid_z = activated(features)
    _, normed_p, sigmoid_p = activated(partner_features)
    act = jnp.concatenate(
        [
            (normed * sigmoid_z).astype(bf16).reshape(-1, channels),
            (normed_p * sigmoid_p).astype(bf16).reshape(-1, channels),
        ],
        axis=0,
    )

    def pieces(name):
        count = len(SETS[name])
        lhs = windows[name].reshape(count * 9 * own, -1)
        out = jnp.dot(lhs, act, preferred_element_type=f32) * SEND_SCALE
        return out.reshape(count, 9, own, channels)

    first = pieces("far").astype(f16)
    first_left = along(first[:2], -1)
    first_right = along(first[2], 1)
    left = along(pieces("left").astype(f16), -1)
    right = along(pieces("right").astype(f16), 1)
    kept = pieces("kept")
    hub = {
        -15: kept[0] + first_left[0].astype(f32),
        15: kept[1] + first_left[1].astype(f32) + first_right.astype(f32),
    }
    far_to_left, far_to_right, extended, filters = lax.optimization_barrier(
        (hub[15].astype(f16), hub[-15].astype(f16), extended, filters)
    )
    far_left = along(far_to_left, -6)
    far_right = along(far_to_right, 6)

    padded = jnp.pad(extended, ((0, 0), (1, 1), (0, 0)))
    grad_act = jnp.zeros((pixels, channels), f32)
    by_tap = filters.reshape(channels, 9, channels).transpose(1, 0, 2)
    for tap_row in range(3):
        for tap_col in range(3):
            window = padded[
                2 - tap_row : 2 - tap_row + height, 2 - tap_col : 2 - tap_col + columns
            ].reshape(-1, channels)
            grad_act = grad_act + jnp.dot(window, by_tap[tap_row * 3 + tap_col], preferred_element_type=f32)

    grad_pre = grad_act.reshape(height, columns, channels) * (
        sigmoid_z * (1.0 + normed * (1.0 - sigmoid_z))
    )
    bias_part = jnp.sum(grad_pre, axis=(0, 1))
    gain_part = jnp.sum(grad_pre * normalized, axis=(0, 1))
    lead = core == 0
    mine = jnp.where(lead, bias_part, gain_part) + swap_cores(jnp.where(lead, gain_part, bias_part))
    left, right, mine = lax.optimization_barrier((left, right, mine))
    every = from_all(mine, CHIPS)
    total = every.sum(axis=0)
    other = swap_cores(total)
    bias_grad, gain_grad = jnp.where(lead, total, other), jnp.where(lead, other, total)
    mean_grad = group_total(norm_gain * bias_grad) / members
    mean_cross = group_total(norm_gain * gain_grad) / members
    grad_in = std_of * (grad_pre * norm_gain - expand(mean_grad, channels) - normalized * expand(mean_cross, channels))
    grad_in = grad_in.astype(bf16)

    for i, h in enumerate(MIDDLE):
        hub[h] = kept[len(FAR) + i] + left[i].astype(f32) + right[i].astype(f32)
    to_left = along(jnp.stack([hub[-6], hub[12], hub[3]], axis=0).astype(f16), -3).astype(f32)
    to_right = along(jnp.stack([hub[6], hub[-12], hub[-3]], axis=0).astype(f16), 3).astype(f32)
    low = hub[-9] + to_left[0] + to_right[1] + far_right.astype(f32)
    high = hub[9] + to_left[1] + to_right[0] + far_left.astype(f32)
    last_left = along(high.astype(f16), -9).astype(f32)
    last_right = along(low.astype(f16), 9).astype(f32)
    near_left, near_right = to_left[2], to_right[2]
    result = hub[0] + near_left + near_right + last_left + last_right
    filter_grad = result.transpose(1, 0, 2).reshape(own, 3, 3, channels) * (1.0 / (SEND_SCALE * all_pixels))
    return (grad_in, filter_grad, gain_grad, bias_grad)


def solution(mesh):
    chips = mesh.shape["rows"] // CORES_PER_CHIP
    torus = Mesh(
        mesh.devices.reshape(mesh.shape["parts"], chips, CORES_PER_CHIP), PARTS_ROWS
    )
    in_specs = (P(PARTS_ROWS, None, None), P(PARTS_ROWS, None, None), P(), P(), P())
    out_specs = (P(PARTS_ROWS, None, None), P(PARTS_ROWS, None, None, None), P("parts"), P("parts"))
    return jax.shard_map(steps, mesh=torus, in_specs=in_specs, out_specs=out_specs, check_vma=False)
```

```python
import jax
import jax.numpy as jnp
from jax import lax
from jax.sharding import Mesh
from jax.sharding import PartitionSpec as P


GROUPS = 32
CHIPS = "chip"
CORES = "core"
ROWS = ("chip", "core")
PARTS_ROWS = ("parts", "chip", "core")
CORES_PER_CHIP = 2
SEND_SCALE = 1.0 / 128.0
SUM_SCALE = 1.0 / 32768.0
LOW_SCALE = 2048.0

epsilon = 1e-06
f32, bf16, f16 = jnp.float32, jnp.bfloat16, jnp.float16

FAR = (-15, 15)
MIDDLE = (-12, -9, -6, -3, 0, 3, 6, 9, 12)
HUBS = FAR + MIDDLE
SETS = {
    "far": (FAR[0] + 1, FAR[1] + 1, FAR[1] - 1),
    "left": tuple(h + 1 for h in MIDDLE),
    "right": tuple(h - 1 for h in MIDDLE),
    "kept": HUBS,
}


def swap_cores(x):
    return lax.ppermute(x, CORES, [(0, 1), (1, 0)])


def along(x, step):
    chips = lax.axis_size(CHIPS)
    return lax.ppermute(x, CHIPS, [(i, (i + step) % chips) for i in range(chips)])


def from_all(vector, axes):
    copies = jnp.broadcast_to(vector, (lax.axis_size(axes), *vector.shape))
    return lax.all_to_all(copies, axes, split_axis=0, concat_axis=0, tiled=True)


def with_halo(block):
    count = lax.axis_size(ROWS)
    forward = [(i, i + 1) for i in range(count - 1)]
    backward = [(target, source) for source, target in forward]
    low = lax.ppermute(block[-1:], ROWS, forward)
    high = lax.ppermute(block[:1], ROWS, backward)
    return jnp.concatenate([low, block, high], axis=0)


def expand(values, channels):
    groups = values.shape[0]
    return jnp.broadcast_to(values[:, None], (groups, channels // groups)).reshape(channels)


def group_total(values):
    return values.reshape(GROUPS, -1).sum(axis=1)


def picked_channels(places, channels, core):
    chips = lax.axis_size(CHIPS)
    own = channels // (chips * CORES_PER_CHIP)
    column = jnp.arange(len(places) * own)
    place = jnp.repeat(jnp.array(places), own)
    owner = (lax.axis_index(CHIPS) - place + 2 * chips) % chips
    channel = (owner * CORES_PER_CHIP + core) * own + column % own
    return (jnp.arange(channels)[:, None] == channel[None, :]).astype(bf16)


def column_shifts(rows, columns):
    flat = rows.shape[1]
    at = lax.broadcasted_iota(jnp.int32, rows.shape, 1) % columns
    edge = jnp.zeros((rows.shape[0], 1), rows.dtype)
    ahead = jnp.concatenate([rows[:, 1:], edge], axis=1)
    behind = jnp.concatenate([edge, rows[:, : flat - 1]], axis=1)
    zero = jnp.zeros((), rows.dtype)
    return (
        jnp.where(at == columns - 1, zero, ahead),
        rows,
        jnp.where(at == 0, zero, behind),
    )


def coded(sums):
    scaled = sums * SUM_SCALE
    high = scaled.astype(f16)
    low = ((scaled - high.astype(f32)) * LOW_SCALE).astype(f16)
    return jnp.pad(jnp.concatenate([high, low], axis=0), ((0, 8 - 2 * sums.shape[0]), (0, 0)))[None]


def decoded(tile, count):
    wide = tile.astype(f32)
    return (wide[:count] + wide[count : 2 * count] * (1.0 / LOW_SCALE)) * (1.0 / SUM_SCALE)


def send(terms, sums, step):
    own, channels = terms.shape[-2:]
    packed = jnp.concatenate([terms.reshape(-1, own, channels), coded(sums)], axis=0)
    got = along(packed, step)
    return got[:-1].reshape(terms.shape), decoded(got[-1], sums.shape[0])


def steps(features, grad_out, filters, norm_gain, norm_bias):
    height, columns, channels = features.shape
    chips = lax.axis_size(CHIPS)
    pixels = height * columns
    all_pixels = pixels * chips * CORES_PER_CHIP
    members = all_pixels * (channels // GROUPS)
    own = channels // (chips * CORES_PER_CHIP)
    core = lax.axis_index(CORES)

    widened = features.astype(f32)
    partial_value = jnp.sum(widened, axis=(0, 1))
    squares = jnp.sum(widened * widened, axis=(0, 1))
    stats = jnp.concatenate([group_total(partial_value), group_total(squares)])
    all_stats = from_all(stats, ROWS)

    extended = with_halo(grad_out)
    partner_features = swap_cores(features)
    flat = extended.reshape(-1, channels)
    places = sum(SETS.values(), ())
    chosen = jnp.concatenate(
        [picked_channels(places, channels, core), picked_channels(places, channels, 1 - core)], axis=1
    )
    rows = lax.dot_general(chosen, flat, (((0,), (1,)), ((), ())), preferred_element_type=f32).astype(bf16)
    half = len(places) * own
    both = (rows[:half], swap_cores(rows[half:]))
    lines = [b[:, k * columns : (k + 1) * columns] for k in range(height + 2) for b in both]
    shifted = column_shifts(jnp.concatenate(lines, axis=1), columns)
    windows, at = {}, 0
    for name, set_places in SETS.items():
        end = at + len(set_places) * own
        windows[name] = jnp.concatenate([x[at:end] for x in shifted], axis=0)
        at = end
    late_windows = windows.pop("kept")
    padded = jnp.pad(extended, ((0, 0), (1, 1), (0, 0)))
    grad_act = jnp.zeros((pixels, channels), f32)
    by_tap = filters.reshape(channels, 9, channels).transpose(1, 0, 2)
    for tap_row in range(3):
        for tap_col in range(3):
            window = padded[
                2 - tap_row : 2 - tap_row + height, 2 - tap_col : 2 - tap_col + columns
            ].reshape(-1, channels)
            grad_act = grad_act + jnp.dot(window, by_tap[tap_row * 3 + tap_col], preferred_element_type=f32)

    all_stats, grad_act, windows, partner_features = lax.optimization_barrier(
        (all_stats, grad_act, windows, partner_features)
    )

    stats = all_stats.sum(axis=0)
    group_mean = stats[:GROUPS] / members
    group_var = stats[GROUPS:] / members - group_mean * group_mean
    inv_std = lax.rsqrt(group_var + epsilon)
    mean_of, std_of = expand(group_mean, channels), expand(inv_std, channels)

    def activated(block):
        normalized = (block.astype(f32) - mean_of) * std_of
        normed = normalized * norm_gain + norm_bias
        return normalized, normed, jax.nn.sigmoid(normed)

    normalized, normed, sigmoid_z = activated(features)
    _, normed_p, sigmoid_p = activated(partner_features)
    act = jnp.stack([(normed * sigmoid_z).astype(bf16), (normed_p * sigmoid_p).astype(bf16)], axis=1)
    act = act.reshape(-1, channels)

    grad_pre = grad_act.reshape(height, columns, channels) * (
        sigmoid_z * (1.0 + normed * (1.0 - sigmoid_z))
    )
    mine = jnp.stack([jnp.sum(grad_pre, axis=(0, 1)), jnp.sum(grad_pre * normalized, axis=(0, 1))])
    sums = mine + swap_cores(mine)

    def pieces(name, dtype):
        count = len(SETS[name])
        taps = []
        for tap_row in range(3):
            lo = (2 - tap_row) * 2 * columns
            lhs = windows[name][:, lo : lo + act.shape[0]]
            out = (jnp.dot(lhs, act, preferred_element_type=f32) * SEND_SCALE).astype(dtype)
            taps.append(out.reshape(3, count, own, channels))
        return jnp.concatenate(taps, axis=0)

    first = pieces("far", f16)
    first_left, sums_right = send(first[:, :2], sums, -1)
    first_right, sums_left = send(first[:, 2], sums, 1)
    left = along(pieces("left", f16), -1)
    right = along(pieces("right", f16), 1)
    windows["kept"] = late_windows
    kept = pieces("kept", f32)
    hub = {
        -15: kept[:, 0] + first_left[:, 0].astype(f32),
        15: kept[:, 1] + first_left[:, 1].astype(f32) + first_right.astype(f32),
    }
    far_to_left, far_to_right, kept = lax.optimization_barrier(
        (hub[15].astype(f16), hub[-15].astype(f16), kept)
    )
    sums_2 = sums + sums_right
    sums_3 = sums_2 + sums_left
    far_left, next_3 = send(far_to_left, sums_3, -3)
    far_right, last_32 = send(far_to_right, jnp.concatenate([sums_3, sums_2]), 3)
    far_left, far_right, next_3, last_32 = lax.optimization_barrier((far_left, far_right, next_3, last_32))
    sums_9 = sums_3 + next_3 + last_32[:2]
    for i, h in enumerate(MIDDLE):
        hub[h] = kept[:, len(FAR) + i] + left[:, i].astype(f32) + right[:, i].astype(f32)
    hub[12] = hub[12] + far_left.astype(f32)
    hub[-12] = hub[-12] + far_right.astype(f32)
    to_left, next_6 = send(jnp.stack([hub[-6], hub[12]], axis=0).astype(f16), next_3, -3)
    to_right, last_6 = send(jnp.stack([hub[6], hub[-12]], axis=0).astype(f16), last_32[2:], 3)
    near_left = along(hub[3].astype(f16), -3)
    near_right = along(hub[-3].astype(f16), 3)
    to_left, to_right, next_6, last_6 = lax.optimization_barrier((to_left, to_right, next_6, last_6))
    to_left, to_right = to_left.astype(f32), to_right.astype(f32)
    low = hub[-9] + to_left[0] + to_right[1]
    high = hub[9] + to_left[1] + to_right[0]
    last_left, ahead_12 = send(high.astype(f16), sums_9 + next_6, -9)
    last_right, behind_11 = send(low.astype(f16), sums_9 + last_6, 9)
    near = hub[0] + near_left.astype(f32) + near_right.astype(f32)
    bias_grad, gain_grad = sums_9 + ahead_12 + behind_11
    group_of = jnp.arange(channels) // (channels // GROUPS)
    same_group = (group_of[:, None] == group_of[None, :]).astype(f32)
    weighted = jnp.stack([norm_gain * bias_grad, norm_gain * gain_grad])
    mean_grad, mean_cross = jnp.dot(weighted, same_group, precision=lax.Precision.HIGHEST) / members
    grad_in = std_of * (
        grad_pre * norm_gain
        - mean_grad
        - normalized * mean_cross
    )
    result = near + last_left.astype(f32) + last_right.astype(f32)
    filter_grad = result.transpose(1, 0, 2).reshape(own, 3, 3, channels) * (1.0 / (SEND_SCALE * all_pixels))
    return (grad_in.astype(bf16), filter_grad, gain_grad, bias_grad)


def solution(mesh):
    chips = mesh.shape["rows"] // CORES_PER_CHIP
    torus = Mesh(
        mesh.devices.reshape(mesh.shape["parts"], chips, CORES_PER_CHIP), PARTS_ROWS
    )
    in_specs = (P(PARTS_ROWS, None, None), P(PARTS_ROWS, None, None), P(), P(), P())
    out_specs = (P(PARTS_ROWS, None, None), P(PARTS_ROWS, None, None, None), P("parts"), P("parts"))
    return jax.shard_map(steps, mesh=torus, in_specs=in_specs, out_specs=out_specs, check_vma=False)
```

```python
import jax
import jax.numpy as jnp
from jax import lax
from jax.sharding import Mesh
from jax.sharding import PartitionSpec as P


GROUPS = 32
CHIPS = "chip"
CORES = "core"
ROWS = ("chip", "core")
PARTS_ROWS = ("parts", "chip", "core")
CORES_PER_CHIP = 2
SEND_SCALE = 1.0 / 128.0
SUM_SCALE = 1.0 / 32768.0
LOW_SCALE = 2048.0

epsilon = 1e-06
f32, bf16, f16 = jnp.float32, jnp.bfloat16, jnp.float16

FAR = (-15, 15)
MIDDLE = (-12, -9, -6, -3, 0, 3, 6, 9, 12)
HUBS = FAR + MIDDLE
SETS = {
    "far": (FAR[0] + 1, FAR[1] + 1, FAR[1] - 1),
    "left": tuple(h + 1 for h in MIDDLE),
    "right": tuple(h - 1 for h in MIDDLE),
    "kept": HUBS,
}


def swap_cores(x):
    return lax.ppermute(x, CORES, [(0, 1), (1, 0)])


def along(x, step):
    chips = lax.axis_size(CHIPS)
    return lax.ppermute(x, CHIPS, [(i, (i + step) % chips) for i in range(chips)])


def from_all(vector, axes):
    copies = jnp.broadcast_to(vector, (lax.axis_size(axes), *vector.shape))
    return lax.all_to_all(copies, axes, split_axis=0, concat_axis=0, tiled=True)


def with_halo(block):
    count = lax.axis_size(ROWS)
    forward = [(i, i + 1) for i in range(count - 1)]
    backward = [(target, source) for source, target in forward]
    low = lax.ppermute(block[-1:], ROWS, forward)
    high = lax.ppermute(block[:1], ROWS, backward)
    return jnp.concatenate([low, block, high], axis=0)


def expand(values, channels):
    groups = values.shape[0]
    return jnp.broadcast_to(values[:, None], (groups, channels // groups)).reshape(channels)


def group_total(values):
    return values.reshape(GROUPS, -1).sum(axis=1)


def picked_channels(places, channels, core):
    chips = lax.axis_size(CHIPS)
    own = channels // (chips * CORES_PER_CHIP)
    column = jnp.arange(len(places) * own)
    place = jnp.repeat(jnp.array(places), own)
    owner = (lax.axis_index(CHIPS) - place + 2 * chips) % chips
    channel = (owner * CORES_PER_CHIP + core) * own + column % own
    return (jnp.arange(channels)[:, None] == channel[None, :]).astype(bf16)


def column_shifts(rows, columns):
    flat = rows.shape[1]
    at = lax.broadcasted_iota(jnp.int32, rows.shape, 1) % columns
    edge = jnp.zeros((rows.shape[0], 1), rows.dtype)
    ahead = jnp.concatenate([rows[:, 1:], edge], axis=1)
    behind = jnp.concatenate([edge, rows[:, : flat - 1]], axis=1)
    zero = jnp.zeros((), rows.dtype)
    return (
        jnp.where(at == columns - 1, zero, ahead),
        rows,
        jnp.where(at == 0, zero, behind),
    )


def coded(sums):
    scaled = sums * SUM_SCALE
    high = lax.reduce_precision(scaled, exponent_bits=5, mantissa_bits=10)
    low = (scaled - high) * LOW_SCALE
    return jnp.pad(jnp.concatenate([high, low], axis=0), ((0, 8 - 2 * sums.shape[0]), (0, 0))).astype(f16)[None]


def decoded(tile, count):
    wide = tile.astype(f32)
    return (wide[:count] + wide[count : 2 * count] * (1.0 / LOW_SCALE)) * (1.0 / SUM_SCALE)


def send(terms, sums, step):
    own, channels = terms.shape[-2:]
    packed = jnp.concatenate([terms.reshape(-1, own, channels), coded(sums)], axis=0)
    got = along(packed, step)
    return got[:-1].reshape(terms.shape), decoded(got[-1], sums.shape[0])


def steps(features, grad_out, filters, norm_gain, norm_bias):
    height, columns, channels = features.shape
    chips = lax.axis_size(CHIPS)
    pixels = height * columns
    all_pixels = pixels * chips * CORES_PER_CHIP
    members = all_pixels * (channels // GROUPS)
    own = channels // (chips * CORES_PER_CHIP)
    core = lax.axis_index(CORES)

    widened = features.astype(f32)
    partial_value = jnp.sum(widened, axis=(0, 1))
    squares = jnp.sum(widened * widened, axis=(0, 1))
    stats = jnp.concatenate([group_total(partial_value), group_total(squares)])
    all_stats = from_all(stats, ROWS)

    extended = with_halo(grad_out)
    partner_features = swap_cores(features)
    flat = extended.reshape(-1, channels)
    places = sum(SETS.values(), ())
    chosen = jnp.concatenate(
        [picked_channels(places, channels, core), picked_channels(places, channels, 1 - core)], axis=1
    )
    rows = lax.dot_general(chosen, flat, (((0,), (1,)), ((), ())), preferred_element_type=f32).astype(bf16)
    half = len(places) * own
    both = (rows[:half], swap_cores(rows[half:]))
    lines = [b[:, k * columns : (k + 1) * columns] for k in range(height + 2) for b in both]
    shifted = column_shifts(jnp.concatenate(lines, axis=1), columns)
    windows, at = {}, 0
    for name, set_places in SETS.items():
        end = at + len(set_places) * own
        windows[name] = jnp.concatenate([x[at:end] for x in shifted], axis=0)
        at = end
    padded = jnp.pad(extended, ((0, 0), (1, 1), (0, 0)))
    grad_act = jnp.zeros((pixels, channels), f32)
    by_tap = filters.reshape(channels, 9, channels).transpose(1, 0, 2)
    for tap_row in range(3):
        for tap_col in range(3):
            window = padded[
                2 - tap_row : 2 - tap_row + height, 2 - tap_col : 2 - tap_col + columns
            ].reshape(-1, channels)
            grad_act = grad_act + jnp.dot(window, by_tap[tap_row * 3 + tap_col], preferred_element_type=f32)

    all_stats, grad_act, windows, partner_features = lax.optimization_barrier(
        (all_stats, grad_act, windows, partner_features)
    )

    stats = all_stats.sum(axis=0)
    group_mean = stats[:GROUPS] / members
    group_var = stats[GROUPS:] / members - group_mean * group_mean
    inv_std = lax.rsqrt(group_var + epsilon)
    mean_of, std_of = expand(group_mean, channels), expand(inv_std, channels)

    def activated(block):
        normalized = (block.astype(f32) - mean_of) * std_of
        normed = normalized * norm_gain + norm_bias
        return normalized, normed, jax.nn.sigmoid(normed)

    normalized, normed, sigmoid_z = activated(features)
    _, normed_p, sigmoid_p = activated(partner_features)
    act = jnp.stack([(normed * sigmoid_z).astype(bf16), (normed_p * sigmoid_p).astype(bf16)], axis=1)
    act = act.reshape(-1, channels)

    grad_pre = grad_act.reshape(height, columns, channels) * (
        sigmoid_z * (1.0 + normed * (1.0 - sigmoid_z))
    )
    mine = jnp.stack([jnp.sum(grad_pre, axis=(0, 1)), jnp.sum(grad_pre * normalized, axis=(0, 1))])
    sums = mine + swap_cores(mine)

    def pieces(name, dtype):
        count = len(SETS[name])
        taps = []
        for tap_row in range(3):
            lo = (2 - tap_row) * 2 * columns
            lhs = windows[name][:, lo : lo + act.shape[0]]
            out = (jnp.dot(lhs, act, preferred_element_type=f32) * SEND_SCALE).astype(dtype)
            taps.append(out.reshape(3, count, own, channels))
        return jnp.concatenate(taps, axis=0)

    first = pieces("far", f16)
    first_left, sums_right = send(first[:, :2], sums, -1)
    first_right, sums_left = send(first[:, 2], sums, 1)
    left = along(pieces("left", f16), -1)
    right = along(pieces("right", f16), 1)
    kept = pieces("kept", f32)
    hub = {
        -15: kept[:, 0] + first_left[:, 0].astype(f32),
        15: kept[:, 1] + first_left[:, 1].astype(f32) + first_right.astype(f32),
    }
    far_to_left, far_to_right, kept = lax.optimization_barrier(
        (hub[15].astype(f16), hub[-15].astype(f16), kept)
    )
    sums_2 = sums + sums_right
    sums_3 = sums_2 + sums_left
    far_left, next_3 = send(far_to_left, sums_3, -3)
    far_right, last_32 = send(far_to_right, jnp.concatenate([sums_3, sums_2]), 3)
    far_left, far_right, next_3, last_32 = lax.optimization_barrier((far_left, far_right, next_3, last_32))
    sums_9 = sums_3 + next_3 + last_32[:2]
    for i, h in enumerate(MIDDLE):
        hub[h] = kept[:, len(FAR) + i] + left[:, i].astype(f32) + right[:, i].astype(f32)
    hub[12] = hub[12] + far_left.astype(f32)
    hub[-12] = hub[-12] + far_right.astype(f32)
    to_left, next_6 = send(jnp.stack([hub[-6], hub[12], hub[3]], axis=0).astype(f16), next_3, -3)
    to_right, last_6 = send(jnp.stack([hub[6], hub[-12], hub[-3]], axis=0).astype(f16), last_32[2:], 3)
    to_left, to_right, next_6, last_6 = lax.optimization_barrier((to_left, to_right, next_6, last_6))
    to_left, to_right = to_left.astype(f32), to_right.astype(f32)
    low = hub[-9] + to_left[0] + to_right[1]
    high = hub[9] + to_left[1] + to_right[0]
    last_left, ahead_12 = send(high.astype(f16), sums_9 + next_6, -9)
    last_right, behind_11 = send(low.astype(f16), sums_9 + last_6, 9)
    near = hub[0] + to_left[2] + to_right[2]
    bias_grad, gain_grad = sums_9 + ahead_12 + behind_11
    group_of = jnp.arange(channels) // (channels // GROUPS)
    same_group = (group_of[:, None] == group_of[None, :]).astype(f32)
    weighted = jnp.stack([norm_gain * bias_grad, norm_gain * gain_grad])
    mean_grad, mean_cross = jnp.dot(weighted, same_group, precision=lax.Precision.HIGHEST) / members
    grad_in = std_of * (
        grad_pre * norm_gain
        - mean_grad
        - normalized * mean_cross
    )
    result = near + last_left.astype(f32) + last_right.astype(f32)
    filter_grad = result.transpose(1, 0, 2).reshape(own, 3, 3, channels) * (1.0 / (SEND_SCALE * all_pixels))
    return (grad_in.astype(bf16), filter_grad, gain_grad, bias_grad)


def solution(mesh):
    chips = mesh.shape["rows"] // CORES_PER_CHIP
    torus = Mesh(
        mesh.devices.reshape(mesh.shape["parts"], chips, CORES_PER_CHIP), PARTS_ROWS
    )
    in_specs = (P(PARTS_ROWS, None, None), P(PARTS_ROWS, None, None), P(), P(), P())
    out_specs = (P(PARTS_ROWS, None, None), P(PARTS_ROWS, None, None, None), P("parts"), P("parts"))
    return jax.shard_map(steps, mesh=torus, in_specs=in_specs, out_specs=out_specs, check_vma=False)
```
